32 devices in a mesh: row: 8 (over y, x, core), col: 4 (over z).
Axes of the slice: x: 2, y: 2, z: 4, core: 2. Of those that a mesh axis runs over, the one named last changes fastest.
Arguments:
- points: bfloat16 [4096, 128], P(('row', 'col')), may hold values from -6 to 6
- abar: bfloat16 [4096, 8, 4, 128], P('row', None, 'col'), may hold values from -6 to 6
- inv_scale: float32 [128], replicated, may hold values from 0.05 to 0.2
Outputs:
- point_grad: float32 [4096, 128], P(('row', 'col'))
The draws below stay inside these ranges and needn't reach their ends.
All inputs are finite; a program needn't handle non-finite values.
Results may differ from the reference program's by a relative error of at most 0.0052.
Values may be sent and summed in bfloat16 or wider, within the bound.
A program may use at most 64 MiB of HBM per device.

```python
import math
import jax
import jax.numpy as jnp
from jax import lax

FEAT = 128
PTS = 128
NPTS = 4096
N_ROW = 8
N_COL = 4


def with_spikes(values, key, source, target, parts, factor):
    owner, partner = [(jnp.arange(values.shape[dim]) // (values.shape[dim] // parts)).reshape([-1 if axis == dim else 1 for axis in range(values.ndim)]) for dim in (source, target)]
    chosen = jax.random.permutation(key, parts)[partner]
    strong = (owner == chosen) | (owner == (partner + parts // 2) % parts)
    return jnp.where(strong, factor * values, values)


def level_of(own_key, shape, cuts, least, high):
    level, own = 1.0, jax.random.fold_in(own_key, 6)
    for axis_at, parts in cuts:
        heights = jnp.exp(jax.random.uniform(jax.random.fold_in(own, axis_at), (parts,), jnp.float32, least / len(cuts), high / len(cuts)))
        level = level * jnp.repeat(heights, shape[axis_at] // parts).reshape([-1 if axis == axis_at else 1 for axis in range(len(shape))])
    return level


def normal_values(own_key, shape, width, reach, split=(), held_as=jnp.bfloat16):
    values = width * jax.random.normal(own_key, shape, jnp.float32)
    if split:
        values = values * level_of(own_key, shape, split, -0.22, 0.18)
    return jnp.clip(values, -reach, reach).astype(held_as)


def gaussian_with(key, shape, deviation, limit, shards, heavy, kind=jnp.bfloat16):
    drawn = deviation * jax.random.normal(key, shape, jnp.float32)
    if shards:
        drawn = drawn * level_of(key, shape, shards, -0.22, 0.18)
    return jnp.clip(with_spikes(drawn, jax.random.fold_in(key, 3), *heavy), -limit, limit).astype(kind)


def setup_inputs(seed: int = 0) -> dict:
    keys = jax.random.split(jax.random.key(seed), 4)
    return {
        "points": normal_values(keys[0], (NPTS, FEAT), 1.0, 6.0, ((0, 32),)),
        "abar": gaussian_with(keys[1], (NPTS, N_ROW, N_COL, PTS), 1.0, 6.0, ((0, 8), (2, 4)), (2, 0, 4, 2.0)),
        "inv_scale": jnp.clip(jnp.exp(jax.random.uniform(keys[2], (FEAT,), jnp.float32, math.log(0.05), math.log(0.2))), 0.05, 0.2),
    }


def reference(points, abar, inv_scale):
    scaled = (points.astype(jnp.float32) * inv_scale[None, :]).astype(jnp.bfloat16)
    wide = scaled.astype(jnp.float32)
    squares = jnp.sum(wide * wide, axis=1)
    matrix = abar.reshape(NPTS, NPTS)
    block = 512 if NPTS % 512 == 0 else NPTS
    count = NPTS // block

    def one_block(carry, index):
        col_acc, col_total = carry
        start = (index * block).astype(jnp.int32)
        rows_scaled = lax.dynamic_slice_in_dim(scaled, start, block, 0)
        rows_sq = lax.dynamic_slice_in_dim(squares, start, block, 0)
        rows_ab = lax.dynamic_slice_in_dim(matrix, start, block, 0)
        inner = lax.dot_general(rows_scaled, scaled, (((1,), (1,)), ((), ())), preferred_element_type=jnp.float32)
        dist = rows_sq[:, None] + squares[None, :] - 2.0 * inner
        weighted = (rows_ab.astype(jnp.float32) * jnp.exp(-0.5 * dist)).astype(jnp.bfloat16)
        row_total = jnp.sum(weighted, axis=1, dtype=jnp.float32)
        first = row_total[:, None] * rows_scaled.astype(jnp.float32) - jnp.dot(weighted, scaled, preferred_element_type=jnp.float32)
        col_acc = col_acc + lax.dot_general(weighted, rows_scaled, (((0,), (0,)), ((), ())), preferred_element_type=jnp.float32)
        col_total = col_total + jnp.sum(weighted, axis=0, dtype=jnp.float32)
        return (col_acc, col_total), first

    init = (jnp.zeros((NPTS, FEAT), jnp.float32), jnp.zeros((NPTS,), jnp.float32))
    (col_acc, col_total), firsts = lax.scan(one_block, init, jnp.arange(count, dtype=jnp.int32))
    first = firsts.reshape(NPTS, FEAT)
    second = col_total[:, None] * wide - col_acc
    return -(first + second) * inv_scale[None, :]
```

```python
import functools

import jax
import jax.numpy as jnp
from jax import lax
from jax.experimental import pallas as pl
from jax.experimental.pallas import tpu as pltpu
from jax.sharding import PartitionSpec as P

MESH = pl.DeviceIdType.MESH
F32, BF16 = jnp.float32, jnp.bfloat16


def augment(block, left):
    wide = block.astype(F32)
    half = -0.5 * jnp.sum(wide * wide, axis=1, keepdims=True)
    high = half.astype(BF16).astype(F32)
    mid = (half - high).astype(BF16).astype(F32)
    low = half - high - mid
    lane = lax.broadcasted_iota(jnp.int32, wide.shape, 1)
    shift = 0 if left else 3
    parts = jnp.where(lane == shift, high, 0.0)
    parts = jnp.where(lane == shift + 1, mid, parts)
    parts = jnp.where(lane == shift + 2, low, parts)
    ones = (lane >= 3 - shift) & (lane < 6 - shift)
    parts = jnp.where(ones, 1.0, parts)
    return jnp.concatenate([block, parts.astype(BF16)], axis=1)


def partner(index, k, count):
    if count & (count - 1):
        return lax.rem(index + k, count)
    out, bit = 0, 1
    while bit < count:
        digit = (index // bit) % 2
        out = out + bit * ((1 - digit) if k & bit else digit)
        bit *= 2
    return out


def returns_to(index, k, count):
    if count & (count - 1):
        return lax.rem(index + count - k, count)
    return partner(index, k, count)


def kernel(
    n_row, n_col, pts_hbm, inv_hbm, ab_hbm, out_ref,
    pts_v, inv_v, ab_v, af, scaled_v, rows_v, cols_v, left, right, row_one, col_one, acc, sec,
    first_out, second_out, first_in, second_in,
    load_sem, rows_send, rows_recv, cols_send, cols_recv,
    first_send, first_recv, second_send, second_recv,
):
    r, c = lax.axis_index("row"), lax.axis_index("col")
    size, feat = pts_v.shape
    rows = n_col * size
    row_to = [partner(r, k, n_row) for k in range(n_row)]
    col_to = [partner(c, k, n_col) for k in range(n_col)]
    row_from = [returns_to(r, k, n_row) for k in range(n_row)]
    col_from = [returns_to(c, k, n_col) for k in range(n_col)]

    barrier = pltpu.get_barrier_semaphore()
    for k in reversed(range(1, n_col)):
        pl.semaphore_signal(barrier, inc=1, device_id=(r, col_to[k]), device_id_type=MESH)
    for k in reversed(range(1, n_row)):
        pl.semaphore_signal(barrier, inc=1, device_id=(row_to[k], c), device_id_type=MESH)
    loads = [
        pltpu.make_async_copy(src, dst, load_sem.at[k])
        for k, (src, dst) in enumerate([(pts_hbm, pts_v), (inv_hbm, inv_v), (ab_hbm, ab_v)])
    ]
    for load in loads:
        load.start()
    loads[0].wait()
    loads[1].wait()
    scaled = (pts_v[...].astype(F32) * inv_v[...]).astype(BF16)
    scaled_v[...] = scaled

    pl.semaphore_wait(barrier, n_col + n_row - 2)

    def send(src, dst, send_sem, recv_sem, device):
        return pltpu.make_async_remote_copy(
            src_ref=src, dst_ref=dst, send_sem=send_sem, recv_sem=recv_sem,
            device_id=device, device_id_type=MESH,
        )

    def row_copy(k):
        return send(scaled_v, rows_v.at[k], rows_send.at[k], rows_recv.at[k], (r, col_to[k]))

    def col_copy(k):
        return send(scaled_v, cols_v.at[k], cols_send.at[k], cols_recv.at[k], (row_to[k], c))

    def first_copy(k):
        return send(
            first_out.at[k], first_in.at[k], first_send.at[k], first_recv.at[k], (r, col_from[k])
        )

    def second_copy(k):
        return send(
            second_out.at[k], second_in.at[k], second_send.at[k], second_recv.at[k], (row_from[k], c)
        )

    for k in reversed(range(1, n_col)):
        row_copy(k).start()
    for k in reversed(range(1, n_row)):
        col_copy(k).start()

    ones = jnp.ones((size, feat), BF16)

    def place_row(k, block):
        left[k * size : (k + 1) * size] = augment(block, True)
        row_one[k * size : (k + 1) * size] = jnp.concatenate([block, ones], axis=1)

    def place_col(k, block):
        right[k * size : (k + 1) * size] = augment(block, False)
        col_one[k * size : (k + 1) * size] = jnp.concatenate([block, ones], axis=1)

    place_row(0, scaled)
    place_col(0, scaled)
    loads[2].wait()
    step = min(rows, 128)

    def widen(i, carry):
        at = pl.multiple_of(i * step, step)
        part = ab_v[pl.ds(at, step)].astype(F32)
        af[pl.ds(pl.multiple_of(at * n_row, step), step * n_row)] = part.reshape(step * n_row, size)
        return carry

    lax.fori_loop(0, rows // step, widen, 0)
    acc[...] = jnp.zeros_like(acc)
    sec[...] = jnp.zeros_like(sec)
    def compute(r0, r1, c0, c1):
        if r0 >= r1:
            return
        for k in range(c0, c1, 2):
            some = range(k, min(k + 2, c1))
            lo, hi = k * size, (some[-1] + 1) * size
            exponent = lax.dot_general(
                left[r0 * size : r1 * size], right[lo:hi], (((1,), (1,)), ((), ())),
                preferred_element_type=F32,
            )
            factors = jnp.concatenate([
                jnp.concatenate([
                    af[pl.ds(col_from[i] * (size * n_row) + row_from[j], size, stride=n_row), :]
                    for i in range(r0, r1)
                ], axis=0)
                for j in some
            ], axis=1)
            weighted = (factors * jnp.exp(exponent)).astype(BF16)
            acc[r0 * size : r1 * size] += jnp.dot(
                weighted, col_one[lo:hi], preferred_element_type=F32
            )
            sec[lo:hi] += lax.dot_general(
                weighted, row_one[r0 * size : r1 * size], (((0,), (0,)), ((), ())),
                preferred_element_type=F32,
            )

    def finish(total, one, k):
        both = total[k * size : (k + 1) * size]
        block = one[k * size : (k + 1) * size, :feat].astype(F32)
        return both[:, feat:] * block - both[:, :feat]

    near_r, near_c = max(1, n_row), max(1, n_col)
    for k in range(1, near_c):
        row_copy(k).wait_recv()
    for k in range(1, near_r):
        col_copy(k).wait_recv()
    for k in range(1, near_c):
        place_row(k, rows_v[k])
    for k in range(1, near_r):
        place_col(k, cols_v[k])
    compute(0, near_c, 0, near_r)
    for k in range(near_c, n_col):
        row_copy(k).wait_recv()
    for k in range(near_r, n_row):
        col_copy(k).wait_recv()
    for k in range(near_c, n_col):
        place_row(k, rows_v[k])
    for k in range(near_r, n_row):
        place_col(k, cols_v[k])
    compute(0, n_col, near_r, n_row)
    compute(near_c, n_col, 0, near_r)

    pending = None
    for k in reversed(range(1, n_col)):
        first_out[k] = finish(acc, row_one, k).astype(BF16)
        if pending is not None:
            pending.start()
        pending = first_copy(k)
    for k in reversed(range(1, n_row)):
        second_out[k] = finish(sec, col_one, k).astype(BF16)
        if pending is not None:
            pending.start()
        pending = second_copy(k)
    total = finish(acc, row_one, 0) + finish(sec, col_one, 0)
    out_ref[...] = total
    if pending is not None:
        pending.start()
    for k in range(1, n_row):
        second_copy(k).wait_recv()
    for k in range(1, n_col):
        first_copy(k).wait_recv()
    for k in range(1, n_row):
        total = total + second_in[k].astype(F32)
    for k in range(1, n_col):
        total = total + first_in[k].astype(F32)
    out_ref[...] = total * -inv_v[...]
    for k in range(1, n_col):
        row_copy(k).wait_send()
        first_copy(k).wait_send()
    for k in range(1, n_row):
        col_copy(k).wait_send()
        second_copy(k).wait_send()


def per_device(n_row, n_col, points, abar, inv_scale):
    size, feat = points.shape
    rows = abar.shape[0]
    dma = pltpu.SemaphoreType.DMA
    any_space = pl.BlockSpec(memory_space=pl.ANY)
    total = pl.pallas_call(
        functools.partial(kernel, n_row, n_col),
        out_shape=pltpu.VMEM((size, feat), F32),
        in_specs=[any_space] * 3,
        out_specs=pl.BlockSpec(memory_space=pltpu.VMEM),
        scratch_shapes=[
            pltpu.VMEM((size, feat), BF16),
            pltpu.VMEM((1, feat), F32),
            pltpu.VMEM((rows, n_row, size), BF16),
            pltpu.VMEM((rows * n_row, size), F32),
            pltpu.VMEM((size, feat), BF16),
            pltpu.VMEM((n_col, size, feat), BF16),
            pltpu.VMEM((n_row, size, feat), BF16),
            pltpu.VMEM((rows, 2 * feat), BF16),
            pltpu.VMEM((n_row * size, 2 * feat), BF16),
            pltpu.VMEM((rows, 2 * feat), BF16),
            pltpu.VMEM((n_row * size, 2 * feat), BF16),
            pltpu.VMEM((rows, 2 * feat), F32),
            pltpu.VMEM((n_row * size, 2 * feat), F32),
            pltpu.VMEM((n_col, size, feat), BF16),
            pltpu.VMEM((n_row, size, feat), BF16),
            pltpu.VMEM((n_col, size, feat), BF16),
            pltpu.VMEM((n_row, size, feat), BF16),
            dma((3,)),
            dma((n_col,)), dma((n_col,)), dma((n_row,)), dma((n_row,)),
            dma((n_col,)), dma((n_col,)), dma((n_row,)), dma((n_row,)),
        ],
        compiler_params=pltpu.CompilerParams(collective_id=0, has_side_effects=True),
    )(points, inv_scale.reshape(1, feat), abar.reshape(rows, n_row, size))
    return total


def solution(mesh):
    placed = (P(("row", "col"), None), P("row", None, "col", None), P())
    body = functools.partial(per_device, mesh.shape["row"], mesh.shape["col"])
    return jax.shard_map(
        body, mesh=mesh, in_specs=placed, out_specs=P(("row", "col"), None), check_vma=False
    )
```

```python
import functools

import jax
import jax.numpy as jnp
from jax import lax
from jax.experimental import pallas as pl
from jax.experimental.pallas import tpu as pltpu
from jax.sharding import PartitionSpec as P

MESH = pl.DeviceIdType.MESH
F32, BF16 = jnp.float32, jnp.bfloat16


def partner(index, k, count):
    if count & (count - 1):
        return lax.rem(index + k, count)
    out, bit = 0, 1
    while bit < count:
        one, two = (index // bit) % 2, (k // bit) % 2
        out = out + bit * (one + two - 2 * one * two)
        bit *= 2
    return out


def returns_to(index, k, count):
    if count & (count - 1):
        return lax.rem(index + count - k, count)
    return partner(index, k, count)


def half_square(block):
    wide = block.astype(F32)
    return -0.5 * jnp.sum(wide * wide, axis=1, keepdims=True)


def marks(size, feat, first):
    lane = lax.broadcasted_iota(jnp.int32, (size, feat), 1)
    return jnp.where((lane >= first) & (lane < first + 3), 1.0, 0.0).astype(BF16)


def augment(block, left):
    half = half_square(block)
    high = half.astype(BF16).astype(F32)
    mid = (half - high).astype(BF16).astype(F32)
    low = half - high - mid
    lane = lax.broadcasted_iota(jnp.int32, block.shape, 1)
    shift = 0 if left else 3
    parts = jnp.where(lane == shift, high, 0.0)
    parts = jnp.where(lane == shift + 1, mid, parts)
    parts = jnp.where(lane == shift + 2, low, parts)
    ones = (lane >= 3 - shift) & (lane < 6 - shift)
    return jnp.where(ones, 1.0, parts).astype(BF16)


def kernel(
    n_row, n_col, pts_hbm, inv_hbm, ab_hbm, out_ref,
    pts_v, inv_v, ab_v, af, rows_v, cols_v, left_aug, right_aug, row_t, col_t,
    weighted, acc, sec,
    first_out, second_out, first_in, second_in,
    load_sem, rows_send, rows_recv, cols_send, cols_recv,
    first_send, first_recv, second_send, second_recv,
):
    r, c = lax.axis_index("row"), lax.axis_index("col")
    size, feat = pts_v.shape
    rows = n_col * size
    row_to = [partner(r, k, n_row) for k in range(n_row)]
    col_to = [partner(c, k, n_col) for k in range(n_col)]
    row_from = [returns_to(r, k, n_row) for k in range(n_row)]
    col_from = [returns_to(c, k, n_col) for k in range(n_col)]

    barrier = pltpu.get_barrier_semaphore()
    for k in reversed(range(1, n_col)):
        pl.semaphore_signal(barrier, inc=1, device_id=(r, col_to[k]), device_id_type=MESH)
    for k in reversed(range(1, n_row)):
        pl.semaphore_signal(barrier, inc=1, device_id=(row_to[k], c), device_id_type=MESH)
    loads = [
        pltpu.make_async_copy(src, dst, load_sem.at[k])
        for k, (src, dst) in enumerate([(pts_hbm, pts_v), (inv_hbm, inv_v), (ab_hbm, ab_v)])
    ]
    for load in loads:
        load.start()
    loads[0].wait()
    loads[1].wait()
    own = (pts_v[...].astype(F32) * inv_v[...]).astype(BF16)
    rows_v[0] = own
    cols_v[0] = own
    pl.semaphore_wait(barrier, n_col + n_row - 2)

    def send(src, dst, send_sem, recv_sem, device):
        return pltpu.make_async_remote_copy(
            src_ref=src, dst_ref=dst, send_sem=send_sem, recv_sem=recv_sem,
            device_id=device, device_id_type=MESH,
        )

    def row_copy(k):
        return send(rows_v.at[0], rows_v.at[k], rows_send.at[k], rows_recv.at[k], (r, partner(c, k, n_col)))

    def col_copy(k):
        return send(rows_v.at[0], cols_v.at[k], cols_send.at[k], cols_recv.at[k], (row_to[k], c))

    def first_copy(k):
        return send(
            first_out.at[k], first_in.at[k], first_send.at[k], first_recv.at[k],
            (r, returns_to(c, k, n_col)),
        )

    def second_copy(k):
        return send(
            second_out.at[k], second_in.at[k], second_send.at[k], second_recv.at[k], (row_from[k], c)
        )

    def farthest_first(copy_of):
        if n_col & (n_col - 1):
            for k in range(1, n_col):
                copy_of(k).start()
            return
        for d in reversed(range(1, n_col)):
            @pl.when(c >= d)
            def _():
                copy_of(partner(c, c - d, n_col)).start()

            @pl.when(c + d < n_col)
            def _():
                copy_of(partner(c, c + d, n_col)).start()

    for k in reversed(range(1, n_row)):
        col_copy(k).start()
    farthest_first(row_copy)

    left_aug[0] = augment(own, True)
    right_aug[0] = augment(own, False)
    own_t = own.T
    col_t[0] = own_t
    loads[2].wait()
    step = min(rows, 128)

    def widen(i, carry):
        at = pl.multiple_of(i * step, step)
        part = ab_v[pl.ds(at, step)].astype(F32)
        af[pl.ds(pl.multiple_of(at * n_row, step), step * n_row)] = part.reshape(step * n_row, size)
        return carry

    lax.fori_loop(0, rows // step, widen, 0)

    early = n_col
    late = list(range(early, n_col))
    wide = n_row * size
    extra = row_t.shape[0] - feat
    groups = [(k, min(k + 2, n_row)) for k in range(0, n_row, 2)]
    cut = (len(groups) + 1) // 2
    chunks = [groups[:1] + groups[cut + 1 :], groups[1 : cut + 1]]

    def joined(block, other):
        return jnp.concatenate([block, other], axis=1)

    def stack(parts):
        return jnp.concatenate(parts, axis=0) if len(parts) > 1 else parts[0]

    def weigh(some_rows, left, half, groups):
        top, low = some_rows[0] * size, (some_rows[-1] + 1) * size
        for begin, end in groups:
            right = stack([joined(cols_v[j], right_aug[j]) for j in range(begin, end)])
            exponent = lax.dot_general(
                left, right, (((1,), (1,)), ((), ())), preferred_element_type=F32
            )
            if half is not None:
                exponent = exponent + half
            factors = jnp.concatenate([
                stack([
                    af[pl.ds(col_from[i] * (size * n_row) + row_from[j], size, stride=n_row), :]
                    for i in some_rows
                ])
                for j in range(begin, end)
            ], axis=1)
            weighted[top:low, begin * size : end * size] = (
                factors * jnp.exp(exponent)
            ).astype(BF16)
        spans = [(begin * size, end * size) for begin, end in groups]
        block = jnp.concatenate([weighted[top:low, begin:end] for begin, end in spans], axis=1)
        every = stack([
            joined(cols_v[j], jnp.ones((size, feat), BF16))
            for begin, end in groups for j in range(begin, end)
        ])
        by_row = jnp.dot(block, every, preferred_element_type=F32)
        by_col = jnp.dot(row_t[:, top:low], block, preferred_element_type=F32)
        return by_row, by_col

    def finish(both, block):
        return both[:, feat:] * block.astype(F32) - both[:, :feat]

    row_t[feat:] = jnp.ones((extra, rows), BF16)
    row_t[:feat, :size] = own_t
    for k in range(1, early):
        row_copy(k).wait_recv()
    for k in range(1, early):
        left_aug[k] = augment(rows_v[k], True)
        row_t[:feat, k * size : (k + 1) * size] = rows_v[k].T
    pending = [None]

    def queue(copy):
        if pending[0] is not None:
            pending[0].start()
        pending[0] = copy

    def turned(k):
        both = sec[:, k * size : (k + 1) * size]
        return both[feat : feat + 1] * col_t[k].astype(F32) - both[:feat]

    for at, chunk in enumerate(chunks):
        members = [k for begin, end in chunk for k in range(begin, end)]
        for k in members:
            if k:
                col_copy(k).wait_recv()
        for k in members:
            if k:
                right_aug[k] = augment(cols_v[k], False)
                col_t[k] = cols_v[k].T
        by_row, by_col = weigh(
            list(range(early)),
            stack([joined(rows_v[i], left_aug[i]) for i in range(early)]), None, chunk,
        )
        if at == 0:
            acc[...] = by_row
        else:
            acc[...] += by_row
        for n, k in enumerate(members):
            sec[:, k * size : (k + 1) * size] = by_col[:, n * size : (n + 1) * size]
        if at == len(chunks) - 1:
            for k in range(1, early):
                first_out[k] = finish(acc[k * size : (k + 1) * size], rows_v[k]).astype(BF16)
            if pending[0] is not None:
                queue(None)
            farthest_first(first_copy)
        for k in reversed(members):
            if k:
                second_out[k] = turned(k).astype(BF16)
                queue(second_copy(k))
    total = finish(acc[:size], rows_v[0])
    total_t = turned(0)
    out_ref[...] = total
    queue(None)
    for k in range(1, early):
        first_copy(k).wait_recv()
        total = total + first_in[k].astype(F32)
    for k in reversed(range(1, n_row)):
        second_copy(k).wait_recv()
        total_t = total_t + second_in[k].astype(F32)
    total = total + total_t.T
    for k in late:
        first_copy(k).wait_recv()
        total = total + first_in[k].astype(F32)
    out_ref[...] = total * -inv_v[...]
    for k in range(1, n_col):
        row_copy(k).wait_send()
        first_copy(k).wait_send()
    for k in range(1, n_row):
        col_copy(k).wait_send()
        second_copy(k).wait_send()


def per_device(n_row, n_col, points, abar, inv_scale):
    size, feat = points.shape
    rows = abar.shape[0]
    dma = pltpu.SemaphoreType.DMA
    any_space = pl.BlockSpec(memory_space=pl.ANY)
    total = pl.pallas_call(
        functools.partial(kernel, n_row, n_col),
        out_shape=pltpu.VMEM((size, feat), F32),
        in_specs=[any_space] * 3,
        out_specs=pl.BlockSpec(memory_space=pltpu.VMEM),
        scratch_shapes=[
            pltpu.VMEM((size, feat), BF16),
            pltpu.VMEM((1, feat), F32),
            pltpu.VMEM((rows, n_row, size), BF16),
            pltpu.VMEM((rows * n_row, size), F32),
            pltpu.VMEM((n_col, size, feat), BF16),
            pltpu.VMEM((n_row, size, feat), BF16),
            pltpu.VMEM((n_col, size, feat), BF16),
            pltpu.VMEM((n_row, size, feat), BF16),
            pltpu.VMEM((feat + 16, rows), BF16),
            pltpu.VMEM((n_row, feat, size), BF16),
            pltpu.VMEM((rows, n_row * size), BF16),
            pltpu.VMEM((n_col * size, 2 * feat), F32),
            pltpu.VMEM((feat + 16, n_row * size), F32),
            pltpu.VMEM((n_col, size, feat), BF16),
            pltpu.VMEM((n_row, feat, size), BF16),
            pltpu.VMEM((n_col, size, feat), BF16),
            pltpu.VMEM((n_row, feat, size), BF16),
            dma((3,)),
            dma((n_col,)), dma((n_col,)), dma((n_row,)), dma((n_row,)),
            dma((n_col,)), dma((n_col,)), dma((n_row,)), dma((n_row,)),
        ],
        compiler_params=pltpu.CompilerParams(collective_id=0, has_side_effects=True),
    )(points, inv_scale.reshape(1, feat), abar.reshape(rows, n_row, size))
    return total


def solution(mesh):
    placed = (P(("row", "col"), None), P("row", None, "col", None), P())
    body = functools.partial(per_device, mesh.shape["row"], mesh.shape["col"])
    return jax.shard_map(
        body, mesh=mesh, in_specs=placed, out_specs=P(("row", "col"), None), check_vma=False
    )
```

```python
import functools

import jax
import jax.numpy as jnp
from jax import lax
from jax.experimental import pallas as pl
from jax.experimental.pallas import tpu as pltpu
from jax.sharding import PartitionSpec as P

MESH = pl.DeviceIdType.MESH
F32, BF16 = jnp.float32, jnp.bfloat16


def partner(index, k, count):
    if count & (count - 1):
        return lax.rem(index + k, count)
    out, bit = 0, 1
    while bit < count:
        one, two = (index // bit) % 2, (k // bit) % 2
        out = out + bit * (one + two - 2 * one * two)
        bit *= 2
    return out


def returns_to(index, k, count):
    if count & (count - 1):
        return lax.rem(index + count - k, count)
    return partner(index, k, count)


def half_square(block):
    wide = block.astype(F32)
    return -0.5 * jnp.sum(wide * wide, axis=1, keepdims=True)


def marks(size, feat, first):
    lane = lax.broadcasted_iota(jnp.int32, (size, feat), 1)
    return jnp.where((lane >= first) & (lane < first + 3), 1.0, 0.0).astype(BF16)


def augment(block):
    half = half_square(block)
    high = half.astype(BF16).astype(F32)
    mid = (half - high).astype(BF16).astype(F32)
    low = half - high - mid
    lane = lax.broadcasted_iota(jnp.int32, block.shape, 1)
    parts = jnp.where(lane == 0, high, 0.0)
    parts = jnp.where(lane == 1, mid, parts)
    return jnp.where(lane == 2, low, parts).astype(BF16)


def kernel(
    n_row, n_col, pts_hbm, inv_hbm, ab_hbm, out_ref,
    pts_v, inv_v, ab_v, af, rows_v, cols_v, left_aug, col_half, row_t, col_t,
    weighted, acc, sec,
    first_out, second_out, first_in, second_in,
    load_sem, rows_send, rows_recv, cols_send, cols_recv,
    first_send, first_recv, second_send, second_recv,
):
    r, c = lax.axis_index("row"), lax.axis_index("col")
    size, feat = pts_v.shape
    rows = n_col * size
    row_to = [partner(r, k, n_row) for k in range(n_row)]
    col_to = [partner(c, k, n_col) for k in range(n_col)]
    row_from = [returns_to(r, k, n_row) for k in range(n_row)]
    col_from = [returns_to(c, k, n_col) for k in range(n_col)]

    barrier = pltpu.get_barrier_semaphore()
    for k in reversed(range(1, n_col)):
        pl.semaphore_signal(barrier, inc=1, device_id=(r, col_to[k]), device_id_type=MESH)
    for k in reversed(range(1, n_row)):
        pl.semaphore_signal(barrier, inc=1, device_id=(row_to[k], c), device_id_type=MESH)
    loads = [
        pltpu.make_async_copy(src, dst, load_sem.at[k])
        for k, (src, dst) in enumerate([(pts_hbm, pts_v), (inv_hbm, inv_v), (ab_hbm, ab_v)])
    ]
    for load in loads:
        load.start()
    loads[0].wait()
    loads[1].wait()
    own = (pts_v[...].astype(F32) * inv_v[...]).astype(BF16)
    rows_v[0] = own
    cols_v[0] = own
    pl.semaphore_wait(barrier, n_col + n_row - 2)

    def send(src, dst, send_sem, recv_sem, device):
        return pltpu.make_async_remote_copy(
            src_ref=src, dst_ref=dst, send_sem=send_sem, recv_sem=recv_sem,
            device_id=device, device_id_type=MESH,
        )

    def row_copy(k):
        return send(rows_v.at[0], rows_v.at[k], rows_send.at[k], rows_recv.at[k], (r, partner(c, k, n_col)))

    def col_copy(k):
        return send(rows_v.at[0], cols_v.at[k], cols_send.at[k], cols_recv.at[k], (row_to[k], c))

    def first_copy(k):
        return send(
            first_out.at[k], first_in.at[k], first_send.at[k], first_recv.at[k],
            (r, returns_to(c, k, n_col)),
        )

    def second_copy(k):
        return send(
            second_out.at[k], second_in.at[k], second_send.at[k], second_recv.at[k], (row_from[k], c)
        )

    def farthest_first(copy_of):
        if n_col & (n_col - 1):
            for k in range(1, n_col):
                copy_of(k).start()
            return
        for d in reversed(range(1, n_col)):
            @pl.when(c >= d)
            def _():
                copy_of(partner(c, c - d, n_col)).start()

            @pl.when(c + d < n_col)
            def _():
                copy_of(partner(c, c + d, n_col)).start()

    first_cols = [k for k in reversed(range(1, n_row)) if k >= n_row - 2]
    for k in first_cols:
        col_copy(k).start()
    farthest_first(row_copy)
    for k in reversed(range(1, n_row)):
        if k not in first_cols:
            col_copy(k).start()

    left_aug[0] = augment(own)

    def place_col(k, block):
        turned_block = block.T
        wide_block = turned_block.astype(F32)
        col_t[k] = turned_block
        col_half[k] = -0.5 * jnp.sum(wide_block * wide_block, axis=0, keepdims=True)

    place_col(0, own)
    loads[2].wait()
    step = min(rows, 128)

    def widen(i, carry):
        at = pl.multiple_of(i * step, step)
        part = ab_v[pl.ds(at, step)].astype(F32)
        af[pl.ds(pl.multiple_of(at * n_row, step), step * n_row)] = part.reshape(step * n_row, size)
        return carry

    lax.fori_loop(0, rows // step, widen, 0)

    early = n_col
    wide = n_row * size
    extra = row_t.shape[0] - feat
    groups = [(k, min(k + 2, n_row)) for k in range(0, n_row, 2)]
    cut = (len(groups) + 1) // 2
    chunks = [groups[:1] + groups[cut + 1 :], groups[1 : cut + 1]]

    def joined(block, other):
        return jnp.concatenate([block, other], axis=1)

    def stack(parts):
        return jnp.concatenate(parts, axis=0) if len(parts) > 1 else parts[0]

    def weigh(some_rows, left, groups):
        top, low = some_rows[0] * size, (some_rows[-1] + 1) * size
        for begin, end in groups:
            right = stack([joined(cols_v[j], marks(size, feat, 0)) for j in range(begin, end)])
            exponent = lax.dot_general(
                left, right, (((1,), (1,)), ((), ())), preferred_element_type=F32
            )
            halves = [col_half[j] for j in range(begin, end)]
            exponent = exponent + jnp.concatenate(halves, axis=1)
            factors = jnp.concatenate([
                stack([
                    af[pl.ds(col_from[i] * (size * n_row) + row_from[j], size, stride=n_row), :]
                    for i in some_rows
                ])
                for j in range(begin, end)
            ], axis=1)
            weighted[top:low, begin * size : end * size] = (
                factors * jnp.exp(exponent)
            ).astype(BF16)
        spans = [(begin * size, end * size) for begin, end in groups]
        block = jnp.concatenate([weighted[top:low, begin:end] for begin, end in spans], axis=1)
        every = stack([
            joined(cols_v[j], jnp.ones((size, feat), BF16))
            for begin, end in groups for j in range(begin, end)
        ])
        by_row = jnp.dot(block, every, preferred_element_type=F32)
        by_col = jnp.dot(row_t[:, top:low], block, preferred_element_type=F32)
        return by_row, by_col

    def finish(both, block):
        return both[:, feat:] * block.astype(F32) - both[:, :feat]

    row_t[feat:] = jnp.ones((extra, rows), BF16)
    row_t[:feat, :size] = own.T
    for k in range(1, early):
        row_copy(k).wait_recv()
    for k in range(1, early):
        left_aug[k] = augment(rows_v[k])
        row_t[:feat, k * size : (k + 1) * size] = rows_v[k].T
    pending = [None]

    def queue(copy):
        if pending[0] is not None:
            pending[0].start()
        pending[0] = copy

    def turned(k):
        both = sec[:, k * size : (k + 1) * size]
        return both[feat : feat + 1] * col_t[k].astype(F32) - both[:feat]

    for at, chunk in enumerate(chunks):
        members = [k for begin, end in chunk for k in range(begin, end)]
        for k in members:
            if k:
                col_copy(k).wait_recv()
        for k in members:
            if k:
                place_col(k, cols_v[k])
        by_row, by_col = weigh(
            list(range(early)),
            stack([joined(rows_v[i], left_aug[i]) for i in range(early)]), chunk,
        )
        if at == 0:
            acc[...] = by_row
        else:
            acc[...] += by_row
        for n, k in enumerate(members):
            sec[:, k * size : (k + 1) * size] = by_col[:, n * size : (n + 1) * size]
        if at == len(chunks) - 1:
            for k in range(1, early):
                first_out[k] = finish(acc[k * size : (k + 1) * size], rows_v[k]).astype(BF16)
            if pending[0] is not None:
                queue(None)
            farthest_first(first_copy)
        for k in reversed(members):
            if k:
                second_out[k] = turned(k).astype(BF16)
                queue(second_copy(k))
    total = finish(acc[:size], rows_v[0])
    total_t = turned(0)
    out_ref[...] = total
    queue(None)
    for k in range(1, early):
        first_copy(k).wait_recv()
        total = total + first_in[k].astype(F32)
    for k in reversed(range(1, n_row)):
        second_copy(k).wait_recv()
        total_t = total_t + second_in[k].astype(F32)
    total = total + total_t.T
    out_ref[...] = total * -inv_v[...]
    for k in range(1, n_col):
        row_copy(k).wait_send()
        first_copy(k).wait_send()
    for k in range(1, n_row):
        col_copy(k).wait_send()
        second_copy(k).wait_send()


def per_device(n_row, n_col, points, abar, inv_scale):
    size, feat = points.shape
    rows = abar.shape[0]
    dma = pltpu.SemaphoreType.DMA
    any_space = pl.BlockSpec(memory_space=pl.ANY)
    total = pl.pallas_call(
        functools.partial(kernel, n_row, n_col),
        out_shape=pltpu.VMEM((size, feat), F32),
        in_specs=[any_space] * 3,
        out_specs=pl.BlockSpec(memory_space=pltpu.VMEM),
        scratch_shapes=[
            pltpu.VMEM((size, feat), BF16),
            pltpu.VMEM((1, feat), F32),
            pltpu.VMEM((rows, n_row, size), BF16),
            pltpu.VMEM((rows * n_row, size), F32),
            pltpu.VMEM((n_col, size, feat), BF16),
            pltpu.VMEM((n_row, size, feat), BF16),
            pltpu.VMEM((n_col, size, feat), BF16),
            pltpu.VMEM((n_row, 1, size), F32),
            pltpu.VMEM((feat + 16, rows), BF16),
            pltpu.VMEM((n_row, feat, size), BF16),
            pltpu.VMEM((rows, n_row * size), BF16),
            pltpu.VMEM((n_col * size, 2 * feat), F32),
            pltpu.VMEM((feat + 16, n_row * size), F32),
            pltpu.VMEM((n_col, size, feat), BF16),
            pltpu.VMEM((n_row, feat, size), BF16),
            pltpu.VMEM((n_col, size, feat), BF16),
            pltpu.VMEM((n_row, feat, size), BF16),
            dma((3,)),
            dma((n_col,)), dma((n_col,)), dma((n_row,)), dma((n_row,)),
            dma((n_col,)), dma((n_col,)), dma((n_row,)), dma((n_row,)),
        ],
        compiler_params=pltpu.CompilerParams(collective_id=0, has_side_effects=True),
    )(points, inv_scale.reshape(1, feat), abar.reshape(rows, n_row, size))
    return total


def solution(mesh):
    placed = (P(("row", "col"), None), P("row", None, "col", None), P())
    body = functools.partial(per_device, mesh.shape["row"], mesh.shape["col"])
    return jax.shard_map(
        body, mesh=mesh, in_specs=placed, out_specs=P(("row", "col"), None), check_vma=False
    )
```

```python
import functools

import jax
import jax.numpy as jnp
from jax import lax
from jax.experimental import pallas as pl
from jax.experimental.pallas import tpu as pltpu
from jax.sharding import PartitionSpec as P

MESH = pl.DeviceIdType.MESH
F32, BF16 = jnp.float32, jnp.bfloat16


def partner(index, k, count):
    if count & (count - 1):
        return lax.rem(index + k, count)
    out, bit = 0, 1
    while bit < count:
        one, two = (index // bit) % 2, (k // bit) % 2
        out = out + bit * (one + two - 2 * one * two)
        bit *= 2
    return out


def returns_to(index, k, count):
    if count & (count - 1):
        return lax.rem(index + count - k, count)
    return partner(index, k, count)


def half_square(block):
    wide = block.astype(F32)
    return -0.5 * jnp.sum(wide * wide, axis=1, keepdims=True)


def marks(size, feat, first):
    lane = lax.broadcasted_iota(jnp.int32, (size, feat), 1)
    return jnp.where((lane >= first) & (lane < first + 3), 1.0, 0.0).astype(BF16)


def augment(block):
    half = half_square(block)
    high = half.astype(BF16).astype(F32)
    mid = (half - high).astype(BF16).astype(F32)
    low = half - high - mid
    lane = lax.broadcasted_iota(jnp.int32, block.shape, 1)
    parts = jnp.where(lane == 0, high, 0.0)
    parts = jnp.where(lane == 1, mid, parts)
    return jnp.where(lane == 2, low, parts).astype(BF16)


def kernel(
    n_row, n_col, pts_hbm, inv_hbm, ab_hbm, out_ref,
    pts_v, inv_v, ab_v, af, rows_v, cols_v, left_aug, col_half, row_t, col_t,
    weighted, acc, sec,
    first_out, second_out, first_in, second_in,
    load_sem, rows_send, rows_recv, cols_send, cols_recv,
    first_send, first_recv, second_send, second_recv,
):
    r, c = lax.axis_index("row"), lax.axis_index("col")
    size, feat = pts_v.shape
    rows = n_col * size
    row_to = [partner(r, k, n_row) for k in range(n_row)]
    col_to = [partner(c, k, n_col) for k in range(n_col)]
    row_from = [returns_to(r, k, n_row) for k in range(n_row)]
    col_from = [returns_to(c, k, n_col) for k in range(n_col)]

    barrier = pltpu.get_barrier_semaphore()
    for k in reversed(range(1, n_col)):
        pl.semaphore_signal(barrier, inc=1, device_id=(r, col_to[k]), device_id_type=MESH)
    for k in reversed(range(1, n_row)):
        pl.semaphore_signal(barrier, inc=1, device_id=(row_to[k], c), device_id_type=MESH)
    loads = [
        pltpu.make_async_copy(src, dst, load_sem.at[k])
        for k, (src, dst) in enumerate([(pts_hbm, pts_v), (inv_hbm, inv_v), (ab_hbm, ab_v)])
    ]
    for load in loads:
        load.start()
    loads[0].wait()
    loads[1].wait()
    own = (pts_v[...].astype(F32) * inv_v[...]).astype(BF16)
    rows_v[0] = own
    cols_v[0] = own
    pl.semaphore_wait(barrier, n_col + n_row - 2)

    def send(src, dst, send_sem, recv_sem, device):
        return pltpu.make_async_remote_copy(
            src_ref=src, dst_ref=dst, send_sem=send_sem, recv_sem=recv_sem,
            device_id=device, device_id_type=MESH,
        )

    def row_copy(k):
        return send(rows_v.at[0], rows_v.at[k], rows_send.at[k], rows_recv.at[k], (r, partner(c, k, n_col)))

    def col_copy(k):
        return send(rows_v.at[0], cols_v.at[k], cols_send.at[k], cols_recv.at[k], (row_to[k], c))

    def first_copy(k):
        return send(
            first_out.at[k], first_in.at[k], first_send.at[k], first_recv.at[k],
            (r, returns_to(c, k, n_col)),
        )

    def second_copy(k):
        return send(
            second_out.at[k], second_in.at[k], second_send.at[k], second_recv.at[k], (row_from[k], c)
        )

    def farthest_first(copy_of):
        if n_col & (n_col - 1):
            for k in range(1, n_col):
                copy_of(k).start()
            return
        for d in reversed(range(1, n_col)):
            @pl.when(c >= d)
            def _():
                copy_of(partner(c, c - d, n_col)).start()

            @pl.when(c + d < n_col)
            def _():
                copy_of(partner(c, c + d, n_col)).start()

    first_cols = [k for k in reversed(range(1, n_row)) if k >= n_row - 2]
    for k in first_cols:
        col_copy(k).start()
    farthest_first(row_copy)
    for k in reversed(range(1, n_row)):
        if k not in first_cols:
            col_copy(k).start()

    left_aug[0] = augment(own)

    def place_col(k, block):
        turned_block = block.T
        wide_block = turned_block.astype(F32)
        col_t[k] = turned_block
        col_half[k] = -0.5 * jnp.sum(wide_block * wide_block, axis=0, keepdims=True)

    place_col(0, own)
    loads[2].wait()
    step = min(rows, 128)

    def widen(i, carry):
        at = pl.multiple_of(i * step, step)
        part = ab_v[pl.ds(at, step)].astype(F32)
        af[pl.ds(pl.multiple_of(at * n_row, step), step * n_row)] = part.reshape(step * n_row, size)
        return carry

    lax.fori_loop(0, rows // step, widen, 0)

    early = n_col
    wide = n_row * size
    extra = row_t.shape[0] - feat
    groups = [(k, min(k + 2, n_row)) for k in range(0, n_row, 2)]
    cut = (len(groups) + 1) // 2
    chunks = [groups[:1] + groups[cut + 1 :], groups[1 : cut + 1]]

    def joined(block, other):
        return jnp.concatenate([block, other], axis=1)

    def stack(parts):
        return jnp.concatenate(parts, axis=0) if len(parts) > 1 else parts[0]

    def weigh(some_rows, left, groups):
        top, low = some_rows[0] * size, (some_rows[-1] + 1) * size
        for begin, end in groups:
            right = stack([joined(cols_v[j], marks(size, feat, 0)) for j in range(begin, end)])
            exponent = lax.dot_general(
                left, right, (((1,), (1,)), ((), ())), preferred_element_type=F32
            )
            halves = [col_half[j] for j in range(begin, end)]
            exponent = exponent + jnp.concatenate(halves, axis=1)
            factors = jnp.concatenate([
                stack([
                    af[pl.ds(col_from[i] * (size * n_row) + row_from[j], size, stride=n_row), :]
                    for i in some_rows
                ])
                for j in range(begin, end)
            ], axis=1)
            weighted[top:low, begin * size : end * size] = (
                factors * jnp.exp(exponent)
            ).astype(BF16)
        spans = [(begin * size, end * size) for begin, end in groups]
        block = jnp.concatenate([weighted[top:low, begin:end] for begin, end in spans], axis=1)
        every = stack([
            joined(cols_v[j], jnp.ones((size, feat), BF16))
            for begin, end in groups for j in range(begin, end)
        ])
        by_row = jnp.dot(block, every, preferred_element_type=F32)
        by_col = jnp.dot(row_t[:, top:low], block, preferred_element_type=F32)
        return by_row, by_col

    def finish(both, block):
        return both[:, feat:] * block.astype(F32) - both[:, :feat]

    row_t[feat:] = jnp.ones((extra, rows), BF16)
    row_t[:feat, :size] = own.T
    for k in range(1, early):
        row_copy(k).wait_recv()
    for k in range(1, early):
        left_aug[k] = augment(rows_v[k])
        row_t[:feat, k * size : (k + 1) * size] = rows_v[k].T
    pending = [None]

    def queue(copy):
        if pending[0] is not None:
            pending[0].start()
        pending[0] = copy

    def turned(k):
        both = sec[:, k * size : (k + 1) * size]
        return both[feat : feat + 1] * col_t[k].astype(F32) - both[:feat]

    for at, chunk in enumerate(chunks):
        members = [k for begin, end in chunk for k in range(begin, end)]
        for k in members:
            if k:
                col_copy(k).wait_recv()
        for k in members:
            if k:
                place_col(k, cols_v[k])
        by_row, by_col = weigh(
            list(range(early)),
            stack([joined(rows_v[i], left_aug[i]) for i in range(early)]), chunk,
        )
        if at == 0:
            acc[...] = by_row
        else:
            acc[...] += by_row
        for n, k in enumerate(members):
            sec[:, k * size : (k + 1) * size] = by_col[:, n * size : (n + 1) * size]
        if at == len(chunks) - 1:
            for k in range(1, early):
                first_out[k] = finish(acc[k * size : (k + 1) * size], rows_v[k]).astype(BF16)
            if pending[0] is not None:
                queue(None)
            farthest_first(first_copy)
        for k in reversed(members):
            if k:
                second_out[k] = turned(k).astype(BF16)
                queue(second_copy(k))
    total = finish(acc[:size], rows_v[0])
    total_t = turned(0)
    out_ref[...] = total
    queue(None)
    for k in reversed(range(1, n_row)):
        second_copy(k).wait_recv()
        total_t = total_t + second_in[k].astype(F32)
    total = total + total_t.T
    for k in range(1, early):
        first_copy(k).wait_recv()
        total = total + first_in[k].astype(F32)
    out_ref[...] = total * -inv_v[...]
    for k in range(1, n_col):
        row_copy(k).wait_send()
        first_copy(k).wait_send()
    for k in range(1, n_row):
        col_copy(k).wait_send()
        second_copy(k).wait_send()


def per_device(n_row, n_col, points, abar, inv_scale):
    size, feat = points.shape
    rows = abar.shape[0]
    dma = pltpu.SemaphoreType.DMA
    any_space = pl.BlockSpec(memory_space=pl.ANY)
    total = pl.pallas_call(
        functools.partial(kernel, n_row, n_col),
        out_shape=pltpu.VMEM((size, feat), F32),
        in_specs=[any_space] * 3,
        out_specs=pl.BlockSpec(memory_space=pltpu.VMEM),
        scratch_shapes=[
            pltpu.VMEM((size, feat), BF16),
            pltpu.VMEM((1, feat), F32),
            pltpu.VMEM((rows, n_row, size), BF16),
            pltpu.VMEM((rows * n_row, size), F32),
            pltpu.VMEM((n_col, size, feat), BF16),
            pltpu.VMEM((n_row, size, feat), BF16),
            pltpu.VMEM((n_col, size, feat), BF16),
            pltpu.VMEM((n_row, 1, size), F32),
            pltpu.VMEM((feat + 16, rows), BF16),
            pltpu.VMEM((n_row, feat, size), BF16),
            pltpu.VMEM((rows, n_row * size), BF16),
            pltpu.VMEM((n_col * size, 2 * feat), F32),
            pltpu.VMEM((feat + 16, n_row * size), F32),
            pltpu.VMEM((n_col, size, feat), BF16),
            pltpu.VMEM((n_row, feat, size), BF16),
            pltpu.VMEM((n_col, size, feat), BF16),
            pltpu.VMEM((n_row, feat, size), BF16),
            dma((3,)),
            dma((n_col,)), dma((n_col,)), dma((n_row,)), dma((n_row,)),
            dma((n_col,)), dma((n_col,)), dma((n_row,)), dma((n_row,)),
        ],
        compiler_params=pltpu.CompilerParams(collective_id=0, has_side_effects=True),
    )(points, inv_scale.reshape(1, feat), abar.reshape(rows, n_row, size))
    return total


def solution(mesh):
    placed = (P(("row", "col"), None), P("row", None, "col", None), P())
    body = functools.partial(per_device, mesh.shape["row"], mesh.shape["col"])
    return jax.shard_map(
        body, mesh=mesh, in_specs=placed, out_specs=P(("row", "col"), None), check_vma=False
    )
```

```python
import functools

import jax
import jax.numpy as jnp
from jax import lax
from jax.experimental import pallas as pl
from jax.experimental.pallas import tpu as pltpu
from jax.sharding import PartitionSpec as P

MESH = pl.DeviceIdType.MESH
F32, BF16 = jnp.float32, jnp.bfloat16


def partner(index, k, count):
    if count & (count - 1):
        return lax.rem(index + k, count)
    out, bit = 0, 1
    while bit < count:
        one, two = (index // bit) % 2, (k // bit) % 2
        out = out + bit * (one + two - 2 * one * two)
        bit *= 2
    return out


def returns_to(index, k, count):
    if count & (count - 1):
        return lax.rem(index + count - k, count)
    return partner(index, k, count)


def half_square(block):
    wide = block.astype(F32)
    return -0.5 * jnp.sum(wide * wide, axis=1, keepdims=True)


def marks(size, feat, first):
    lane = lax.broadcasted_iota(jnp.int32, (size, feat), 1)
    return jnp.where((lane >= first) & (lane < first + 3), 1.0, 0.0).astype(BF16)


def augment(block):
    half = half_square(block)
    high = half.astype(BF16).astype(F32)
    mid = (half - high).astype(BF16).astype(F32)
    low = half - high - mid
    lane = lax.broadcasted_iota(jnp.int32, block.shape, 1)
    parts = jnp.where(lane == 0, high, 0.0)
    parts = jnp.where(lane == 1, mid, parts)
    return jnp.where(lane == 2, low, parts).astype(BF16)


def kernel(
    n_row, n_col, pts_hbm, inv_hbm, ab_hbm, out_ref,
    pts_v, inv_v, ab_v, af, rows_v, cols_v, left_aug, col_half, row_t, col_t,
    weighted, acc, sec,
    first_out, second_out, first_in, second_in,
    load_sem, rows_send, rows_recv, cols_send, cols_recv,
    first_send, first_recv, second_send, second_recv,
):
    r, c = lax.axis_index("row"), lax.axis_index("col")
    size, feat = pts_v.shape
    rows = n_col * size
    row_to = [partner(r, k, n_row) for k in range(n_row)]
    col_to = [partner(c, k, n_col) for k in range(n_col)]
    row_from = [returns_to(r, k, n_row) for k in range(n_row)]
    col_from = [returns_to(c, k, n_col) for k in range(n_col)]

    barrier = pltpu.get_barrier_semaphore()
    for k in reversed(range(1, n_col)):
        pl.semaphore_signal(barrier, inc=1, device_id=(r, col_to[k]), device_id_type=MESH)
    for k in reversed(range(1, n_row)):
        pl.semaphore_signal(barrier, inc=1, device_id=(row_to[k], c), device_id_type=MESH)
    loads = [
        pltpu.make_async_copy(src, dst, load_sem.at[k])
        for k, (src, dst) in enumerate([(pts_hbm, pts_v), (inv_hbm, inv_v), (ab_hbm, ab_v)])
    ]
    for load in loads:
        load.start()
    loads[0].wait()
    loads[1].wait()
    own = (pts_v[...].astype(F32) * inv_v[...]).astype(BF16)
    rows_v[0] = own
    cols_v[0] = own
    pl.semaphore_wait(barrier, n_col + n_row - 2)

    def send(src, dst, send_sem, recv_sem, device):
        return pltpu.make_async_remote_copy(
            src_ref=src, dst_ref=dst, send_sem=send_sem, recv_sem=recv_sem,
            device_id=device, device_id_type=MESH,
        )

    def row_copy(k):
        return send(rows_v.at[0], rows_v.at[k], rows_send.at[k], rows_recv.at[k], (r, partner(c, k, n_col)))

    def col_copy(k):
        return send(rows_v.at[0], cols_v.at[k], cols_send.at[k], cols_recv.at[k], (row_to[k], c))

    def first_copy(k):
        return send(
            first_out.at[k], first_in.at[k], first_send.at[k], first_recv.at[k],
            (r, returns_to(c, k, n_col)),
        )

    def second_copy(k):
        return send(
            second_out.at[k], second_in.at[k], second_send.at[k], second_recv.at[k], (row_from[k], c)
        )

    def farthest_first(copy_of):
        if n_col & (n_col - 1):
            for k in range(1, n_col):
                copy_of(k).start()
            return
        for d in reversed(range(1, n_col)):
            @pl.when(c >= d)
            def _():
                copy_of(partner(c, c - d, n_col)).start()

            @pl.when(c + d < n_col)
            def _():
                copy_of(partner(c, c + d, n_col)).start()

    first_cols = [k for k in reversed(range(1, n_row)) if k >= n_row - 2]
    for k in first_cols:
        col_copy(k).start()
    farthest_first(row_copy)
    for k in reversed(range(1, n_row)):
        if k not in first_cols:
            col_copy(k).start()

    left_aug[0] = augment(own)

    def place_col(k, block):
        turned_block = block.T
        wide_block = turned_block.astype(F32)
        col_t[k] = turned_block
        col_half[k] = -0.5 * jnp.sum(wide_block * wide_block, axis=0, keepdims=True)

    place_col(0, own)
    loads[2].wait()
    step = min(rows, 128)

    def widen(i, carry):
        at = pl.multiple_of(i * step, step)
        part = ab_v[pl.ds(at, step)].astype(F32)
        af[pl.ds(pl.multiple_of(at * n_row, step), step * n_row)] = part.reshape(step * n_row, size)
        return carry

    lax.fori_loop(0, rows // step, widen, 0)

    early = n_col
    wide = n_row * size
    extra = row_t.shape[0] - feat
    groups = [(k, min(k + 2, n_row)) for k in range(0, n_row, 2)]
    cut = (len(groups) + 1) // 2
    chunks = [groups[:1] + groups[cut + 1 :], groups[1 : cut + 1]]

    def joined(block, other):
        return jnp.concatenate([block, other], axis=1)

    def stack(parts):
        return jnp.concatenate(parts, axis=0) if len(parts) > 1 else parts[0]

    def weigh(some_rows, left, groups):
        top, low = some_rows[0] * size, (some_rows[-1] + 1) * size
        for begin, end in groups:
            right = stack([joined(cols_v[j], marks(size, feat, 0)) for j in range(begin, end)])
            exponent = lax.dot_general(
                left, right, (((1,), (1,)), ((), ())), preferred_element_type=F32
            )
            halves = [col_half[j] for j in range(begin, end)]
            exponent = exponent + jnp.concatenate(halves, axis=1)
            factors = jnp.concatenate([
                stack([
                    af[pl.ds(col_from[i] * (size * n_row) + row_from[j], size, stride=n_row), :]
                    for i in some_rows
                ])
                for j in range(begin, end)
            ], axis=1)
            weighted[top:low, begin * size : end * size] = (
                factors * jnp.exp(exponent)
            ).astype(BF16)
        spans = [(begin * size, end * size) for begin, end in groups]
        block = jnp.concatenate([weighted[top:low, begin:end] for begin, end in spans], axis=1)
        every = stack([
            joined(cols_v[j], jnp.ones((size, feat), BF16))
            for begin, end in groups for j in range(begin, end)
        ])
        by_row = jnp.dot(block, every, preferred_element_type=F32)
        return by_row, lambda: jnp.dot(row_t[:, top:low], block, preferred_element_type=F32)

    def finish(both, block):
        return both[:, feat:] * block.astype(F32) - both[:, :feat]

    row_t[feat:] = jnp.ones((extra, rows), BF16)
    row_t[:feat, :size] = own.T
    for k in range(1, early):
        row_copy(k).wait_recv()
    for k in range(1, early):
        left_aug[k] = augment(rows_v[k])
        row_t[:feat, k * size : (k + 1) * size] = rows_v[k].T
    pending = [None]

    def queue(copy):
        if pending[0] is not None:
            pending[0].start()
        pending[0] = copy

    def turned(k):
        both = sec[:, k * size : (k + 1) * size]
        return both[feat : feat + 1] * col_t[k].astype(F32) - both[:feat]

    for at, chunk in enumerate(chunks):
        members = [k for begin, end in chunk for k in range(begin, end)]
        for k in members:
            if k:
                col_copy(k).wait_recv()
        for k in members:
            if k:
                place_col(k, cols_v[k])
        by_row, by_col = weigh(
            list(range(early)),
            stack([joined(rows_v[i], left_aug[i]) for i in range(early)]), chunk,
        )
        if at == 0:
            acc[...] = by_row
        else:
            acc[...] += by_row
        if at == len(chunks) - 1:
            for k in range(1, early):
                first_out[k] = finish(acc[k * size : (k + 1) * size], rows_v[k]).astype(BF16)
            if pending[0] is not None:
                queue(None)
            farthest_first(first_copy)
        by_col = by_col()
        for n, k in enumerate(members):
            sec[:, k * size : (k + 1) * size] = by_col[:, n * size : (n + 1) * size]
        for k in reversed(members):
            if k:
                second_out[k] = turned(k).astype(BF16)
                queue(second_copy(k))
    total = finish(acc[:size], rows_v[0])
    total_t = turned(0)
    out_ref[...] = total
    queue(None)
    for k in reversed(range(1, n_row)):
        second_copy(k).wait_recv()
        total_t = total_t + second_in[k].astype(F32)
    total = total + total_t.T
    for k in range(1, early):
        first_copy(k).wait_recv()
        total = total + first_in[k].astype(F32)
    out_ref[...] = total * -inv_v[...]
    for k in range(1, n_col):
        row_copy(k).wait_send()
        first_copy(k).wait_send()
    for k in range(1, n_row):
        col_copy(k).wait_send()
        second_copy(k).wait_send()


def per_device(n_row, n_col, points, abar, inv_scale):
    size, feat = points.shape
    rows = abar.shape[0]
    dma = pltpu.SemaphoreType.DMA
    any_space = pl.BlockSpec(memory_space=pl.ANY)
    total = pl.pallas_call(
        functools.partial(kernel, n_row, n_col),
        out_shape=pltpu.VMEM((size, feat), F32),
        in_specs=[any_space] * 3,
        out_specs=pl.BlockSpec(memory_space=pltpu.VMEM),
        scratch_shapes=[
            pltpu.VMEM((size, feat), BF16),
            pltpu.VMEM((1, feat), F32),
            pltpu.VMEM((rows, n_row, size), BF16),
            pltpu.VMEM((rows * n_row, size), F32),
            pltpu.VMEM((n_col, size, feat), BF16),
            pltpu.VMEM((n_row, size, feat), BF16),
            pltpu.VMEM((n_col, size, feat), BF16),
            pltpu.VMEM((n_row, 1, size), F32),
            pltpu.VMEM((feat + 16, rows), BF16),
            pltpu.VMEM((n_row, feat, size), BF16),
            pltpu.VMEM((rows, n_row * size), BF16),
            pltpu.VMEM((n_col * size, 2 * feat), F32),
            pltpu.VMEM((feat + 16, n_row * size), F32),
            pltpu.VMEM((n_col, size, feat), BF16),
            pltpu.VMEM((n_row, feat, size), BF16),
            pltpu.VMEM((n_col, size, feat), BF16),
            pltpu.VMEM((n_row, feat, size), BF16),
            dma((3,)),
            dma((n_col,)), dma((n_col,)), dma((n_row,)), dma((n_row,)),
            dma((n_col,)), dma((n_col,)), dma((n_row,)), dma((n_row,)),
        ],
        compiler_params=pltpu.CompilerParams(collective_id=0, has_side_effects=True),
    )(points, inv_scale.reshape(1, feat), abar.reshape(rows, n_row, size))
    return total


def solution(mesh):
    placed = (P(("row", "col"), None), P("row", None, "col", None), P())
    body = functools.partial(per_device, mesh.shape["row"], mesh.shape["col"])
    return jax.shard_map(
        body, mesh=mesh, in_specs=placed, out_specs=P(("row", "col"), None), check_vma=False
    )
```
